256 devices in a mesh: ens: 64 (over z_lo, x, y), row: 2 (over z_hi), col: 2 (over core).
Axes of the slice: x: 4, y: 4, z: 8 (z_hi: 2, z_lo: 4; z = z_hi * 4 + z_lo), core: 2. Of those that a mesh axis runs over, the one named last changes fastest.
Arguments:
- states: float32 [128, 16, 4096], P('ens', None, ('row', 'col')), parts along dimension 0, may hold values from -4 to 4
- jacobian: bfloat16 [262144, 4096], P(('ens', 'row'), 'col'), parts along dimension 0, as said below
- step_sizes: float32 [128, 1], P('ens'), parts along dimension 0, may hold values from 0.75 to 1.5
Outputs:
- new_states: float32 [128, 16, 4096], P('ens', None, ('row', 'col')), parts along dimension 0
The draws below stay inside these ranges and needn't reach their ends.
There are 64 independent parts, one for each index of `ens`. The reference program is written for one: setup_inputs(seed, part) draws one part's arguments, and reference() takes and returns one part's arrays. A program takes and returns all parts, laid end to end along the dimension named above; each array names one. Nothing has to cross between parts.
Inputs may be any that keep to these rules, and one draw needn't show every extreme that they name: `jacobian`: the diagonal lies between -40 and -1 apart from a term as small as the others, whose magnitude is at most 24 / sqrt(4096).
All inputs are finite; a program needn't handle non-finite values.
Results may differ from the reference program's by a relative error of at most 0.0083.
Values may be sent and summed in bfloat16 or wider, within the bound.
No kernel may reach another device: no remote copies, remote signals or barrier semaphores. Data moves between devices by JAX's collectives and lax.ppermute only.
A program may use at most 64 MiB of HBM per device.

```python
import math
import jax
import jax.numpy as jnp
from jax import lax

N = 4096
COLS = 16
BLOCKS = 12
STEPS = 1
BATCH = 2


def draw_jacobian(key, part):
    first_key, second_key = jax.random.split(jax.random.fold_in(key, 11))
    spread = 4.0 / math.sqrt(N)
    rough = jnp.clip(jax.random.normal(first_key, (N, N), jnp.float32), -6.0, 6.0) * spread
    rates = jnp.exp(jax.random.uniform(second_key, (N,), jnp.float32, 0.0, math.log(40.0)))
    return (rough - jnp.diag(rates)).astype(jnp.bfloat16)


def block_scale(key, shape, pieces, low, top_value):
    loudness = 1.0
    for axis_at, parts in pieces:
        steps = jax.random.uniform(jax.random.fold_in(jax.random.fold_in(key, 6), axis_at), (parts,), jnp.float32, low / len(pieces), top_value / len(pieces))
        loudness = loudness * jnp.repeat(jnp.exp(steps), shape[axis_at] // parts).reshape((-1,) + (1,) * (len(shape) - 1 - axis_at))
    return loudness


def gaussian(stream_key, shape, scale, reach, shards=(), held_as=jnp.bfloat16):
    array = scale * jax.random.normal(stream_key, shape, jnp.float32)
    if shards:
        array = array * block_scale(stream_key, shape, shards, -0.22, 0.18)
    return jnp.clip(array, -reach, reach).astype(held_as)


def setup_inputs(seed: int = 0, part: int = 0) -> dict:
    keys = jax.random.split(jax.random.key(seed), 4)
    part_keys = jax.random.split(jax.random.fold_in(keys[3], part), 4)
    return {
        "states": gaussian(part_keys[0], (BATCH, COLS, N), 1.0, 4.0, ((2, 4),), jnp.float32),
        "jacobian": draw_jacobian(jax.random.fold_in(jax.random.fold_in(keys[3], part), 71), part),
        "step_sizes": jnp.clip(jnp.exp(jax.random.uniform(part_keys[2], (BATCH, STEPS), jnp.float32, math.log(0.75), math.log(1.5))), 0.75, 1.5),
    }


precise = lax.Precision.HIGHEST
squarings = 10
taylor_degree = 8

def exponential(matrix):
    scaled = matrix / 2.0 ** squarings
    identity = jnp.eye(matrix.shape[-1], dtype=jnp.float32)
    result = jnp.broadcast_to(identity, matrix.shape)
    for degree in range(taylor_degree, 0, -1):
        result = identity + jnp.matmul(scaled, result, precision=precise) / degree
    for squaring in range(squarings):
        result = jnp.matmul(result, result, precision=precise)
    return result

def apply_full(vectors, matrix):
    rounded = lax.optimization_barrier(vectors.astype(jnp.bfloat16)).astype(jnp.float32)
    return jnp.einsum('bcm,nm->bcn', rounded, matrix, precision=precise)

def reference(states, jacobian, step_sizes):
    matrix = jacobian.astype(jnp.float32)
    members = states.shape[0]
    columns = states.shape[1]
    length = states.shape[2]
    krylov = BLOCKS * columns
    for step_index in range(STEPS):
        forcing = apply_full(states, matrix) - states * states * states / 3.0
        root_gram = jnp.einsum('bpn,bqn->bpq', forcing, forcing, precision=precise)
        root_lower = jnp.linalg.cholesky(root_gram)
        leading = lax.linalg.triangular_solve(root_lower, forcing, left_side=True, lower=True)
        krylov_basis = jnp.zeros((members, krylov, length), jnp.float32).at[:, :columns].set(leading)
        hessenberg = jnp.zeros((members, krylov, krylov), jnp.float32)
        for block_index in range(BLOCKS):
            start = block_index * columns
            current = krylov_basis[:, start:start + columns]
            images = apply_full(current, matrix)
            projection = jnp.einsum('bkn,bqn->bkq', krylov_basis, images, precision=precise)
            hessenberg = hessenberg.at[:, :, start:start + columns].set(projection)
            if block_index + 1 < BLOCKS:
                reduced = images - jnp.einsum('bkq,bkn->bqn', projection, krylov_basis, precision=precise)
                gram_matrix = jnp.einsum('bpn,bqn->bpq', reduced, reduced, precision=precise)
                lower_factor = jnp.linalg.cholesky(gram_matrix)
                next_block = lax.linalg.triangular_solve(lower_factor, reduced, left_side=True, lower=True)
                hessenberg = hessenberg.at[:, start + columns:start + 2 * columns, start:start + columns].set(jnp.swapaxes(lower_factor, 1, 2))
                krylov_basis = krylov_basis.at[:, start + columns:start + 2 * columns].set(next_block)
        step_size = step_sizes[:, step_index][:, None, None]
        augmented = jnp.zeros((members, krylov + columns, krylov + columns), jnp.float32)
        augmented = augmented.at[:, :krylov, :krylov].set(step_size * hessenberg)
        augmented = augmented.at[:, :columns, krylov:].set(step_size * jnp.swapaxes(root_lower, 1, 2))
        exponent = exponential(augmented)
        phi_block = exponent[:, :krylov, krylov:]
        states = states + jnp.einsum('bkq,bkn->bqn', phi_block, krylov_basis, precision=precise)
    return states
```

```python
import jax
import jax.numpy as jnp
from jax import lax
from jax.experimental import pallas as pl
from jax.experimental.pallas import tpu as pltpu
from jax.sharding import PartitionSpec as P

BLOCKS = 12
COLS = 16
KRYLOV = BLOCKS * COLS
AUG = KRYLOV + COLS
SQUARINGS = 10
TILE = 512
VMEM_LIMIT = 24 * 1024 * 1024

NT = (((1,), (1,)), ((), ()))
NN = (((1,), (0,)), ((), ()))
f32 = jnp.float32
bf16 = jnp.bfloat16

VMEM = pl.BlockSpec(memory_space=pltpu.VMEM)
SMEM = pl.BlockSpec(memory_space=pltpu.SMEM)


def dot(a, b, dims):
    return lax.dot_general(a, b, dims, preferred_element_type=f32)


def halves_of(x):
    high = x.astype(bf16)
    low = (x - high.astype(f32)).astype(bf16)
    return high, low


def stacked(x):
    return jnp.concatenate(halves_of(x), axis=0)


def matvec_into(image_ref, own_ref, other_ref, vec_ref, minus_ref=None):
    rows = own_ref.shape[0]

    def tile(i, carry):
        at = pl.ds(pl.multiple_of(i * TILE, TILE), TILE)
        part = dot(own_ref[at, :], vec_ref[0], NT) + dot(other_ref[at, :], vec_ref[1], NT)
        value = jnp.swapaxes(part, 0, 1)
        if minus_ref is not None:
            cells = minus_ref[:, at]
            value = value - cells * cells * cells / 3.0
        image_ref[:, at] = value
        return carry

    lax.fori_loop(0, rows // TILE, tile, 0)


def projected(high, low, image):
    both = stacked(image)
    count = high.shape[0]
    terms = dot(high, both, NT) + dot(low, both, NT)
    padded = -count % 128
    if padded:
        terms = jnp.concatenate([terms, jnp.zeros((padded, 2 * COLS), f32)], axis=0)
    turned = jnp.swapaxes(terms, 0, 1)
    return turned[:COLS] + turned[COLS:]


def factored(gram, offset):
    lane = lax.broadcasted_iota(jnp.int32, (COLS, 128), 1)
    row = lax.broadcasted_iota(jnp.int32, (COLS, 128), 0)
    columns = [jnp.broadcast_to(gram[:, k : k + 1], (COLS, 128)) for k in range(COLS)]
    inverse = jnp.where((lane & (COLS - 1)) == row, 1.0, 0.0).astype(f32)
    lower = jnp.zeros((COLS, 128), f32)
    for k in range(COLS):
        scale = lax.rsqrt(columns[k][k : k + 1, :])
        column = jnp.where(row >= k, columns[k] * scale, 0.0)
        lower = jnp.where(lane == offset + k, column, lower)
        pivot_row = inverse[k : k + 1, :] * scale
        inverse = jnp.where(row == k, pivot_row, inverse - jnp.where(row > k, column, 0.0) * pivot_row)
        for j in range(k + 1, COLS):
            columns[j] = columns[j] - column * column[j : j + 1, :]
    return lower, inverse


def gram_of(pairs):
    total = None
    for high, low in pairs:
        first = dot(jnp.concatenate([high, low], axis=0), high, NT)
        part = first[:COLS] + first[COLS:] + dot(high, low, NT)
        total = part if total is None else total + part
    return total


def new_block(reduced, offset, slot, vec_ref, block_ref):
    pairs = [halves_of(r) for r in reduced]
    lower, inverse = factored(gram_of(pairs), offset)
    left = stacked(inverse)[:, : 2 * COLS]
    for side, (high, low) in enumerate(pairs):
        both = dot(left, jnp.concatenate([high, low], axis=0), NN)
        block = both[:COLS] + both[COLS:]
        block_high, block_low = halves_of(block)
        block_ref[side, 0] = block_high
        block_ref[side, 1] = block_low
        vec_ref[slot if side == 0 else 1 - slot] = block_high
    return lower


def basis(blocks, side, piece):
    return jnp.concatenate([b[side, piece] for b in blocks], axis=0)


def first_kernel(slot_ref, own_ref, other_ref, here_ref, away_ref, image_ref, block_ref, row_ref, vec_ref):
    lower = new_block([here_ref[...], away_ref[...]], 0, slot_ref[0], vec_ref, block_ref)
    row_ref[:, :128] = lower
    row_ref[:, 128:] = jnp.zeros((COLS, 128), f32)
    matvec_into(image_ref, own_ref, other_ref, vec_ref)


def orthogonal(away_ref, part_ref, blocks):
    return part_ref[...] + projected(basis(blocks, 1, 0), basis(blocks, 1, 1), away_ref[...])


def turn_kernel(slot_ref, own_ref, other_ref, here_ref, away_ref, part_ref, *refs):
    *blocks, image_ref, block_ref, row_ref, vec_ref = refs
    count = len(blocks) * COLS
    turned = orthogonal(away_ref, part_ref, blocks)
    coefficients = stacked(turned)[:, :count]
    reduced = []
    for side, image in enumerate((here_ref, away_ref)):
        main = dot(coefficients, basis(blocks, side, 0), NN)
        rest = dot(coefficients[:COLS], basis(blocks, side, 1), NN)
        reduced.append(image[...] - (main[:COLS] + main[COLS:] + rest))
    lower = new_block(reduced, count % 128, slot_ref[0], vec_ref, block_ref)
    for tile in (0, 128):
        row = turned[:, tile : tile + 128] if tile < turned.shape[1] else jnp.zeros((COLS, 128), f32)
        row_ref[:, tile : tile + 128] = row + lower if count // 128 * 128 == tile else row
    matvec_into(image_ref, own_ref, other_ref, vec_ref)


def part_kernel(here_ref, *refs):
    *blocks, part_ref = refs
    part_ref[...] = projected(basis(blocks, 0, 0), basis(blocks, 0, 1), here_ref[...])


def product(a, b):
    return lax.dot_general(a, b, NN, precision=lax.Precision.HIGHEST, preferred_element_type=f32)


def last_kernel(step_ref, away_ref, part_ref, *refs):
    blocks, rows, delta_ref = refs[:BLOCKS], refs[BLOCKS:-1], refs[-1]
    turned = orthogonal(away_ref, part_ref, blocks)
    root, *rows = [r[...] for r in rows]
    augmented = jnp.concatenate([*rows, turned, root], axis=0)
    x = augmented[:, :AUG] * (step_ref[0] / 2.0**SQUARINGS)
    row = lax.broadcasted_iota(jnp.int32, (AUG, AUG), 0)
    col = lax.broadcasted_iota(jnp.int32, (AUG, AUG), 1)
    x2 = product(x, x)
    x3 = product(x2, x)
    x4 = product(x2, x2)
    tail = jnp.where(row == col, 1.0 / 24.0, 0.0) + x / 120.0 + x2 / 720.0 + x3 / 5040.0 + x4 / 40320.0
    q = x + x2 / 2.0 + x3 / 6.0 + product(x4, tail)
    for _ in range(SQUARINGS - 1):
        q = 2.0 * q + product(q, q)
    bottom = q[KRYLOV:AUG, :]
    bottom = 2.0 * bottom + product(bottom, q)
    left = stacked(bottom[:, :KRYLOV])
    main = dot(left, basis(blocks, 0, 0), NN)
    delta_ref[...] = main[:COLS] + main[COLS:] + dot(left[:COLS], basis(blocks, 0, 1), NN)


def call(kernel, scalars, arrays, outs, scratch=()):
    return pl.pallas_call(
        kernel,
        out_shape=outs,
        in_specs=[SMEM] * len(scalars) + [VMEM] * len(arrays),
        out_specs=jax.tree.map(lambda _: VMEM, outs),
        scratch_shapes=list(scratch),
        compiler_params=pltpu.CompilerParams(vmem_limit_bytes=VMEM_LIMIT),
    )(*scalars, *arrays)


def shape(*dims, dtype=f32):
    return jax.ShapeDtypeStruct(dims, dtype)


def swap(x, axis):
    return lax.ppermute(x, axis, [(0, 1), (1, 0)])


def local(states, jacobian, step_sizes):
    length = states.shape[2]
    half = 2 * length
    me = lax.axis_index("col")
    other = 1 - me
    slot = (lax.axis_index("row") != me).astype(jnp.int32)[None]

    def take(x, index):
        return lax.dynamic_index_in_dim(x, index, 0, keepdims=False)

    def side_by_side(mine, theirs):
        both = jnp.stack([mine, theirs])
        return jnp.concatenate([take(both, me), take(both, other)], axis=1)

    mine = take(states, me)
    theirs = swap(take(states, other), "col")
    cells = side_by_side(mine, theirs)
    other_jacobian = swap(jacobian, "col")
    rounded = cells.astype(bf16)
    away_rounded = swap(rounded, "row")
    step = take(step_sizes, me)

    scratch = [pltpu.VMEM((2, COLS, half), bf16)]
    image_shape = shape(COLS, half)
    block_shape = shape(2, 2, COLS, half, dtype=bf16)
    row_shape = shape(COLS, 256)

    def force(slot_ref, own_ref, other_ref, here_ref, away_ref, cells_ref, image_ref, vec_ref):
        vec_ref[slot_ref[0]] = here_ref[...]
        vec_ref[1 - slot_ref[0]] = away_ref[...]
        matvec_into(image_ref, own_ref, other_ref, vec_ref, cells_ref)

    tiles = (jacobian, other_jacobian)
    forcing = call(force, (slot,), (*tiles, rounded, away_rounded, cells), image_shape, scratch)
    outs = (image_shape, block_shape, row_shape)
    image, block, row = call(first_kernel, (slot,), (*tiles, forcing, swap(forcing, "row")), outs, scratch)
    blocks, rows = [block], [row]
    for j in range(BLOCKS):
        away = swap(image, "row")
        part = call(part_kernel, (), (image, *blocks), shape(COLS, -(-(j + 1) * COLS // 128) * 128))
        if j + 1 < BLOCKS:
            image, block, row = call(turn_kernel, (slot,), (*tiles, image, away, part, *blocks), outs, scratch)
            blocks.append(block)
            rows.append(row)
    delta = call(last_kernel, (step,), (away, part, *blocks, *rows), image_shape)
    pieces = jnp.stack([delta[:, :length], delta[:, length:]])
    kept = take(pieces, me)
    arrived = swap(take(pieces, other), "col")
    return states + side_by_side_members(kept, arrived, me)


def side_by_side_members(kept, arrived, me):
    first = jnp.where(me == 0, kept, arrived)
    second = jnp.where(me == 0, arrived, kept)
    return jnp.stack([first, second])


def solution(mesh):
    placed = (P("ens", None, ("row", "col")), P(("ens", "row"), "col"), P("ens", None))
    return jax.shard_map(
        local, mesh=mesh, in_specs=placed, out_specs=P("ens", None, ("row", "col")), check_vma=False
    )
```

```python
import jax
import jax.numpy as jnp
from jax import lax
from jax.experimental import pallas as pl
from jax.experimental.pallas import tpu as pltpu
from jax.sharding import PartitionSpec as P

BLOCKS = 12
COLS = 16
KRYLOV = BLOCKS * COLS
AUG = KRYLOV + COLS
SQUARINGS = 10
SCALE = 512.0
TILE = 512
VMEM_LIMIT = 24 * 1024 * 1024

NT = (((1,), (1,)), ((), ()))
NN = (((1,), (0,)), ((), ()))
f32 = jnp.float32
bf16 = jnp.bfloat16

VMEM = pl.BlockSpec(memory_space=pltpu.VMEM)
SMEM = pl.BlockSpec(memory_space=pltpu.SMEM)
FAR = pl.BlockSpec(memory_space=pltpu.HBM)


def dot(a, b, dims):
    return lax.dot_general(a, b, dims, preferred_element_type=f32)


def halves_of(x):
    high = x.astype(bf16)
    low = (x - high.astype(f32)).astype(bf16)
    return high, low


def stacked(x):
    return jnp.concatenate(halves_of(x), axis=0)


def row_tiles(rows, body):
    def tile(i, carry):
        body(i, pl.ds(pl.multiple_of(i * TILE, TILE), TILE))
        return carry

    lax.fori_loop(0, rows // TILE, tile, 0)


def own_kernel(tile_ref, vec_ref, part_ref, own_ref):
    def body(i, at):
        values = tile_ref[at, :]
        own_ref[at, :] = values
        part_ref[:, at] = jnp.swapaxes(dot(values, vec_ref[0], NT), 0, 1)

    row_tiles(own_ref.shape[0], body)


def force_kernel(source_ref, vec_ref, part_ref, cells_ref, image_ref, other_ref, sems):
    count = other_ref.shape[0] // TILE

    def copy(i):
        at = pl.ds(pl.multiple_of(i * TILE, TILE), TILE)
        return pltpu.make_async_copy(source_ref.at[at], other_ref.at[at], sems.at[i])

    copy(0).start()
    copy(1).start()

    def body(i, at):
        copy(i).wait()

        @pl.when(i + 2 < count)
        def _():
            copy(i + 2).start()

        value = part_ref[:, at] + jnp.swapaxes(dot(other_ref[at, :], vec_ref[1], NT), 0, 1)
        cells = cells_ref[:, at]
        image_ref[:, at] = value - cells * cells * cells / 3.0

    row_tiles(other_ref.shape[0], body)


def image_kernel(own_ref, other_ref, vec_ref, image_ref):
    def body(i, at):
        part = dot(own_ref[at, :], vec_ref[0], NT) + dot(other_ref[at, :], vec_ref[1], NT)
        image_ref[:, at] = jnp.swapaxes(part, 0, 1)

    row_tiles(own_ref.shape[0], body)


def projected(high, low, image):
    both = stacked(image)
    count = high.shape[0]
    terms = dot(high, both, NT) + dot(low, both, NT)
    padded = -count % 128
    if padded:
        terms = jnp.concatenate([terms, jnp.zeros((padded, 2 * COLS), f32)], axis=0)
    turned = jnp.swapaxes(terms, 0, 1)
    return turned[:COLS] + turned[COLS:]


def factored(gram, offset):
    lane = lax.broadcasted_iota(jnp.int32, (COLS, 128), 1)
    row = lax.broadcasted_iota(jnp.int32, (COLS, 128), 0)
    columns = [jnp.broadcast_to(gram[:, k : k + 1], (COLS, 128)) for k in range(COLS)]
    inverse = jnp.where((lane & (COLS - 1)) == row, 1.0, 0.0).astype(f32)
    lower = jnp.zeros((COLS, 128), f32)
    for k in range(COLS):
        scale = lax.rsqrt(columns[k][k : k + 1, :])
        column = jnp.where(row >= k, columns[k] * scale, 0.0)
        lower = jnp.where(lane == offset + k, column, lower)
        pivot_row = inverse[k : k + 1, :] * scale
        inverse = jnp.where(row == k, pivot_row, inverse - jnp.where(row > k, column, 0.0) * pivot_row)
        for j in range(k + 1, COLS):
            columns[j] = columns[j] - column * column[j : j + 1, :]
    return lower, inverse


def gram_of(pairs):
    total = None
    for high, low in pairs:
        first = dot(jnp.concatenate([high, low], axis=0), high, NT)
        part = first[:COLS] + first[COLS:] + dot(high, low, NT)
        total = part if total is None else total + part
    return total


def new_block(reduced, offset, slot, vec_ref, block_ref):
    pairs = [halves_of(r) for r in reduced]
    lower, inverse = factored(gram_of(pairs), offset)
    left = stacked(inverse)[:, : 2 * COLS]
    for side, (high, low) in enumerate(pairs):
        both = dot(left, jnp.concatenate([high, low], axis=0), NN)
        block = both[:COLS] + both[COLS:]
        block_high, block_low = halves_of(block)
        block_ref[side, 0] = block_high
        block_ref[side, 1] = block_low
        vec_ref[slot if side == 0 else 1 - slot] = block_high
    return lower


def basis(blocks, side, piece):
    return jnp.concatenate([b[side, piece] for b in blocks], axis=0)


def first_kernel(slot_ref, here_ref, away_ref, block_ref, row_ref, vec_ref):
    lower = new_block([here_ref[...], away_ref[...]], 0, slot_ref[0], vec_ref, block_ref)
    row_ref[:, :128] = lower
    row_ref[:, 128:] = jnp.zeros((COLS, 128), f32)


def orthogonal(away_ref, part_ref, blocks):
    return part_ref[...] + projected(basis(blocks, 1, 0), basis(blocks, 1, 1), away_ref[...])


def turn_kernel(slot_ref, here_ref, away_ref, part_ref, *refs):
    *blocks, block_ref, row_ref, vec_ref = refs
    count = len(blocks) * COLS
    turned = orthogonal(away_ref, part_ref, blocks)
    coefficients = stacked(turned)[:, :count]
    reduced = []
    for side, image in enumerate((here_ref, away_ref)):
        main = dot(coefficients, basis(blocks, side, 0), NN)
        rest = dot(coefficients[:COLS], basis(blocks, side, 1), NN)
        reduced.append(image[...] - (main[:COLS] + main[COLS:] + rest))
    lower = new_block(reduced, count % 128, slot_ref[0], vec_ref, block_ref)
    for tile in (0, 128):
        row = turned[:, tile : tile + 128] if tile < turned.shape[1] else jnp.zeros((COLS, 128), f32)
        row_ref[:, tile : tile + 128] = row + lower if count // 128 * 128 == tile else row


def part_kernel(here_ref, *refs):
    *blocks, part_ref = refs
    part_ref[...] = projected(basis(blocks, 0, 0), basis(blocks, 0, 1), here_ref[...])


def product(a, b):
    rows = a.shape[0]
    high, low = halves_of(b)
    left = stacked(a)
    both = dot(left, high, NN)
    return both[:rows] + both[rows:] + dot(left[:rows], low, NN)


def last_kernel(step_ref, away_ref, part_ref, *refs):
    blocks, rows, delta_ref = refs[:BLOCKS], refs[BLOCKS:-1], refs[-1]
    turned = part_ref[...] + away_ref[...]
    root, *rows = [r[...] for r in rows]
    augmented = jnp.concatenate([*rows, turned, root], axis=0)
    x = augmented[:, :AUG] * (step_ref[0] / 2.0**SQUARINGS)
    row = lax.broadcasted_iota(jnp.int32, (AUG, AUG), 0)
    col = lax.broadcasted_iota(jnp.int32, (AUG, AUG), 1)
    x2 = product(x, x)
    x3 = product(x2, x)
    x4 = product(x2, x2)
    tail = jnp.where(row == col, 1.0 / 24.0, 0.0) + x / 120.0 + x2 / 720.0 + x3 / 5040.0 + x4 / 40320.0
    q = x + x2 / 2.0 + x3 / 6.0 + product(x4, tail)
    q = lax.fori_loop(0, SQUARINGS - 1, lambda _, q: 2.0 * q + product(q, q), q)
    bottom = q[KRYLOV:AUG, :]
    bottom = 2.0 * bottom + product(bottom, q)
    left = stacked(bottom[:, :KRYLOV])
    main = dot(left, basis(blocks, 0, 0), NN)
    delta_ref[...] = main[:COLS] + main[COLS:] + dot(left[:COLS], basis(blocks, 0, 1), NN)


def call(kernel, scalars, arrays, outs, scratch=(), far=()):
    return pl.pallas_call(
        kernel,
        out_shape=outs,
        in_specs=[SMEM] * len(scalars) + [FAR] * len(far) + [VMEM] * len(arrays),
        out_specs=jax.tree.map(lambda _: VMEM, outs),
        scratch_shapes=list(scratch),
        compiler_params=pltpu.CompilerParams(vmem_limit_bytes=VMEM_LIMIT),
    )(*scalars, *far, *arrays)


def shape(*dims, dtype=f32):
    return jax.ShapeDtypeStruct(dims, dtype)


def swap(x, axis):
    return lax.ppermute(x, axis, [(0, 1), (1, 0)])


def local(states, jacobian, step_sizes):
    length = states.shape[2]
    half = 2 * length
    me = lax.axis_index("col")
    other = 1 - me
    slot = (lax.axis_index("row") != me).astype(jnp.int32)[None]

    def take(x, index):
        return lax.dynamic_index_in_dim(x, index, 0, keepdims=False)

    def side_by_side(mine, theirs):
        both = jnp.stack([mine, theirs])
        return jnp.concatenate([take(both, me), take(both, other)], axis=1)

    mine = take(states, me)
    theirs = swap(take(states, other), "col")
    jacobian, theirs = lax.optimization_barrier((jacobian, theirs))
    other_jacobian = swap(jacobian, "col")
    cells = side_by_side(mine, theirs)
    rounded = cells.astype(bf16)
    away_rounded = swap(rounded, "row")
    step = take(step_sizes, me)

    image_shape = shape(COLS, half)
    block_shape = shape(2, 2, COLS, half, dtype=bf16)
    row_shape = shape(COLS, 256)
    vec_shape = shape(2, COLS, half, dtype=bf16)
    outs = (block_shape, row_shape, vec_shape)

    vec = jnp.where(slot[0] == 0, jnp.stack([rounded, away_rounded]), jnp.stack([away_rounded, rounded]))
    tile_shape = shape(*jacobian.shape, dtype=bf16)
    part, own = call(own_kernel, (), (jacobian, vec), (image_shape, tile_shape))
    landing = [pltpu.SemaphoreType.DMA((half // TILE,))]
    forcing, far = call(force_kernel, (), (vec, part, cells), (image_shape, tile_shape), landing, (other_jacobian,))
    block, row, vec = call(first_kernel, (slot,), (forcing, swap(forcing, "row")), outs)
    blocks, rows = [block], [row]
    for j in range(BLOCKS):
        image = call(image_kernel, (), (own, far, vec), image_shape)
        part_shape = shape(COLS, -(-(j + 1) * COLS // 128) * 128)
        if j + 1 < BLOCKS:
            sent = (image * SCALE).astype(jnp.float16)
            image = sent.astype(f32) / SCALE
            away = swap(sent, "row").astype(f32) / SCALE
            part = call(part_kernel, (), (image, *blocks), part_shape)
            block, row, vec = call(turn_kernel, (slot,), (image, away, part, *blocks), outs)
            blocks.append(block)
            rows.append(row)
        else:
            part = call(part_kernel, (), (image, *blocks), part_shape)
            away = swap(part, "row")
    delta = call(last_kernel, (step,), (away, part, *blocks, *rows), image_shape)
    pieces = jnp.stack([delta[:, :length], delta[:, length:]])
    kept = take(pieces, me)
    arrived = swap(take(pieces, other), "col")
    return states + side_by_side_members(kept, arrived, me)


def side_by_side_members(kept, arrived, me):
    first = jnp.where(me == 0, kept, arrived)
    second = jnp.where(me == 0, arrived, kept)
    return jnp.stack([first, second])


def solution(mesh):
    placed = (P("ens", None, ("row", "col")), P(("ens", "row"), "col"), P("ens", None))
    return jax.shard_map(
        local, mesh=mesh, in_specs=placed, out_specs=P("ens", None, ("row", "col")), check_vma=False
    )
```

```python
import jax
import jax.numpy as jnp
from jax import lax
from jax.experimental import pallas as pl
from jax.experimental.pallas import tpu as pltpu
from jax.sharding import PartitionSpec as P

BLOCKS = 12
COLS = 16
KRYLOV = BLOCKS * COLS
AUG = KRYLOV + COLS
SQUARINGS = 10
SCALE = 512.0
TILE = 512
VMEM_LIMIT = 24 * 1024 * 1024

NT = (((1,), (1,)), ((), ()))
NN = (((1,), (0,)), ((), ()))
f32 = jnp.float32
bf16 = jnp.bfloat16

VMEM = pl.BlockSpec(memory_space=pltpu.VMEM)
SMEM = pl.BlockSpec(memory_space=pltpu.SMEM)
FAR = pl.BlockSpec(memory_space=pltpu.HBM)


def dot(a, b, dims):
    return lax.dot_general(a, b, dims, preferred_element_type=f32)


def halves_of(x):
    high = x.astype(bf16)
    low = (x - high.astype(f32)).astype(bf16)
    return high, low


def stacked(x):
    return jnp.concatenate(halves_of(x), axis=0)


def row_tiles(rows, body):
    def tile(i, carry):
        body(i, pl.ds(pl.multiple_of(i * TILE, TILE), TILE))
        return carry

    lax.fori_loop(0, rows // TILE, tile, 0)


def keep_kernel(tile_ref, own_ref):
    def body(i, at):
        own_ref[at, :] = tile_ref[at, :]

    row_tiles(own_ref.shape[0], body)


def own_kernel(own_ref, vec_ref, part_ref):
    def body(i, at):
        part_ref[:, at] = jnp.swapaxes(dot(own_ref[at, :], vec_ref[0], NT), 0, 1)

    row_tiles(own_ref.shape[0], body)


def force_kernel(source_ref, vec_ref, part_ref, cells_ref, image_ref, other_ref, sems):
    count = other_ref.shape[0] // TILE

    def copy(i):
        at = pl.ds(pl.multiple_of(i * TILE, TILE), TILE)
        return pltpu.make_async_copy(source_ref.at[at], other_ref.at[at], sems.at[i])

    copy(0).start()
    copy(1).start()

    def body(i, at):
        copy(i).wait()

        @pl.when(i + 2 < count)
        def _():
            copy(i + 2).start()

        value = part_ref[:, at] + jnp.swapaxes(dot(other_ref[at, :], vec_ref[1], NT), 0, 1)
        cells = cells_ref[:, at]
        image_ref[:, at] = value - cells * cells * cells / 3.0

    row_tiles(other_ref.shape[0], body)


def image_kernel(own_ref, other_ref, vec_ref, image_ref):
    def body(i, at):
        part = dot(own_ref[at, :], vec_ref[0], NT) + dot(other_ref[at, :], vec_ref[1], NT)
        scaled = jnp.swapaxes(part, 0, 1) * SCALE
        wide = scaled * (2.0**13 + 1.0)
        image_ref[:, at] = wide - (wide - scaled)

    row_tiles(own_ref.shape[0], body)


def projected(high, low, image):
    both = stacked(image)
    count = high.shape[0]
    terms = dot(high, both, NT) + dot(low, both, NT)
    padded = -count % 128
    if padded:
        terms = jnp.concatenate([terms, jnp.zeros((padded, 2 * COLS), f32)], axis=0)
    turned = jnp.swapaxes(terms, 0, 1)
    return turned[:COLS] + turned[COLS:]


def factored(gram, offset):
    lane = lax.broadcasted_iota(jnp.int32, (COLS, 128), 1)
    row = lax.broadcasted_iota(jnp.int32, (COLS, 128), 0)
    columns = [jnp.broadcast_to(gram[:, k : k + 1], (COLS, 128)) for k in range(COLS)]
    inverse = jnp.where((lane & (COLS - 1)) == row, 1.0, 0.0).astype(f32)
    lower = jnp.zeros((COLS, 128), f32)
    for k in range(0, COLS, 2):
        first, second = columns[k], columns[k + 1]
        corner, below, last = first[k : k + 1, :], first[k + 1 : k + 2, :], second[k + 1 : k + 2, :]
        scale = lax.rsqrt(corner)
        below = below * scale
        scale_next = lax.rsqrt(last - below * below)
        first = first * scale
        second = (second - first * below) * scale_next
        for j in range(k + 2, COLS):
            columns[j] = columns[j] - first * first[j : j + 1, :] - second * second[j : j + 1, :]
        lower = jnp.where((lane == offset + k) & (row >= k), first, lower)
        lower = jnp.where((lane == offset + k + 1) & (row > k), second, lower)
        pivot = inverse[k : k + 1, :] * scale
        pivot_next = (inverse[k + 1 : k + 2, :] - below * pivot) * scale_next
        rest = inverse - first * pivot - second * pivot_next
        inverse = jnp.where(row > k + 1, rest, inverse)
        inverse = jnp.where(row == k, pivot, jnp.where(row == k + 1, pivot_next, inverse))
    return lower, inverse


def gram_of(pairs):
    total = None
    for high, low in pairs:
        first = dot(jnp.concatenate([high, low], axis=0), high, NT)
        part = first[:COLS] + first[COLS:] + dot(high, low, NT)
        total = part if total is None else total + part
    return total


def new_block(reduced, offset, slot, vec_ref, block_ref):
    pairs = [halves_of(r) for r in reduced]
    lower, inverse = factored(gram_of(pairs), offset)
    left = stacked(inverse)[:, : 2 * COLS]
    for side, (high, low) in enumerate(pairs):
        both = dot(left, jnp.concatenate([high, low], axis=0), NN)
        block = both[:COLS] + both[COLS:]
        block_high, block_low = halves_of(block)
        block_ref[side, 0] = block_high
        block_ref[side, 1] = block_low
        vec_ref[slot if side == 0 else 1 - slot] = block_high
    return lower


def basis(blocks, side, piece):
    return jnp.concatenate([b[side, piece] for b in blocks], axis=0)


def first_kernel(slot_ref, here_ref, away_ref, block_ref, row_ref, vec_ref):
    lower = new_block([here_ref[...], away_ref[...]], 0, slot_ref[0], vec_ref, block_ref)
    row_ref[:, :128] = lower
    row_ref[:, 128:] = jnp.zeros((COLS, 128), f32)


def orthogonal(away_ref, part_ref, blocks):
    return part_ref[...] + projected(basis(blocks, 1, 0), basis(blocks, 1, 1), away_ref[...] / SCALE)


def turn_kernel(slot_ref, here_ref, away_ref, part_ref, *refs):
    *blocks, block_ref, row_ref, vec_ref = refs
    count = len(blocks) * COLS
    turned = orthogonal(away_ref, part_ref, blocks)
    coefficients = stacked(turned)[:, :count]
    reduced = []
    for side, image in enumerate((here_ref, away_ref)):
        main = dot(coefficients, basis(blocks, side, 0), NN)
        rest = dot(coefficients[:COLS], basis(blocks, side, 1), NN)
        reduced.append(image[...] / SCALE - (main[:COLS] + main[COLS:] + rest))
    lower = new_block(reduced, count % 128, slot_ref[0], vec_ref, block_ref)
    for tile in (0, 128):
        row = turned[:, tile : tile + 128] if tile < turned.shape[1] else jnp.zeros((COLS, 128), f32)
        row_ref[:, tile : tile + 128] = row + lower if count // 128 * 128 == tile else row


def part_kernel(here_ref, *refs):
    *blocks, part_ref = refs
    part_ref[...] = projected(basis(blocks, 0, 0), basis(blocks, 0, 1), here_ref[...] / SCALE)


def product(a, b):
    rows = a.shape[0]
    high, low = halves_of(b)
    left = stacked(a)
    both = dot(left, high, NN)
    return both[:rows] + both[rows:] + dot(left[:rows], low, NN)


def last_kernel(step_ref, away_ref, part_ref, *refs):
    blocks, rows, delta_ref = refs[:BLOCKS], refs[BLOCKS:-1], refs[-1]
    turned = part_ref[...] + away_ref[...]
    root, *rows = [r[...] for r in rows]
    augmented = jnp.concatenate([*rows, turned, root], axis=0)
    x = augmented[:, :AUG] * (step_ref[0] / 2.0**SQUARINGS)
    row = lax.broadcasted_iota(jnp.int32, (AUG, AUG), 0)
    col = lax.broadcasted_iota(jnp.int32, (AUG, AUG), 1)
    x2 = product(x, x)
    x3 = product(x2, x)
    x4 = product(x2, x2)
    tail = jnp.where(row == col, 1.0 / 24.0, 0.0) + x / 120.0 + x2 / 720.0 + x3 / 5040.0 + x4 / 40320.0
    q = x + x2 / 2.0 + x3 / 6.0 + product(x4, tail)
    q = lax.fori_loop(0, SQUARINGS - 1, lambda _, q: 2.0 * q + product(q, q), q)
    bottom = q[KRYLOV:AUG, :]
    bottom = 2.0 * bottom + product(bottom, q)
    left = stacked(bottom[:, :KRYLOV])
    main = dot(left, basis(blocks, 0, 0), NN)
    delta_ref[...] = main[:COLS] + main[COLS:] + dot(left[:COLS], basis(blocks, 0, 1), NN)


def call(kernel, scalars, arrays, outs, scratch=(), far=()):
    return pl.pallas_call(
        kernel,
        out_shape=outs,
        in_specs=[SMEM] * len(scalars) + [FAR] * len(far) + [VMEM] * len(arrays),
        out_specs=jax.tree.map(lambda _: VMEM, outs),
        scratch_shapes=list(scratch),
        compiler_params=pltpu.CompilerParams(vmem_limit_bytes=VMEM_LIMIT),
    )(*scalars, *far, *arrays)


def shape(*dims, dtype=f32):
    return jax.ShapeDtypeStruct(dims, dtype)


def swap(x, axis):
    return lax.ppermute(x, axis, [(0, 1), (1, 0)])


def advanced(states, jacobian, step_sizes):
    length = states.shape[2]
    half = 2 * length
    me = lax.axis_index("col")
    other = 1 - me
    slot = (lax.axis_index("row") != me).astype(jnp.int32)[None]

    def take(x, index):
        return lax.dynamic_index_in_dim(x, index, 0, keepdims=False)

    def side_by_side(mine, theirs):
        both = jnp.stack([mine, theirs])
        return jnp.concatenate([take(both, me), take(both, other)], axis=1)

    mine = take(states, me)
    theirs = swap(take(states, other), "col")
    jacobian, theirs = lax.optimization_barrier((jacobian, theirs))
    other_jacobian = swap(jacobian, "col")
    cells = side_by_side(mine, theirs)
    rounded = cells.astype(bf16)
    away_rounded = swap(rounded, "row")
    step = take(step_sizes, me)

    image_shape = shape(COLS, half)
    block_shape = shape(2, 2, COLS, half, dtype=bf16)
    row_shape = shape(COLS, 256)
    vec_shape = shape(2, COLS, half, dtype=bf16)
    outs = (block_shape, row_shape, vec_shape)

    vec = jnp.where(slot[0] == 0, jnp.stack([rounded, away_rounded]), jnp.stack([away_rounded, rounded]))
    tile_shape = shape(*jacobian.shape, dtype=bf16)
    own = call(keep_kernel, (), (jacobian,), tile_shape)
    part = call(own_kernel, (), (own, vec), image_shape)
    landing = [pltpu.SemaphoreType.DMA((half // TILE,))]
    forcing, far = call(force_kernel, (), (vec, part, cells), (image_shape, tile_shape), landing, (other_jacobian,))
    block, row, vec = call(first_kernel, (slot,), (forcing, swap(forcing, "row")), outs)
    blocks, rows = [block], [row]
    for j in range(BLOCKS):
        image = call(image_kernel, (), (own, far, vec), image_shape)
        part_shape = shape(COLS, -(-(j + 1) * COLS // 128) * 128)
        if j + 1 < BLOCKS:
            away = swap(image.astype(jnp.float16), "row").astype(f32)
            part = call(part_kernel, (), (image, *blocks), part_shape)
            block, row, vec = call(turn_kernel, (slot,), (image, away, part, *blocks), outs)
            blocks.append(block)
            rows.append(row)
        else:
            part = call(part_kernel, (), (image, *blocks), part_shape)
            away = swap(part, "row")
    delta = call(last_kernel, (step,), (away, part, *blocks, *rows), image_shape)
    pieces = jnp.stack([delta[:, :length], delta[:, length:]])
    kept = take(pieces, me)
    arrived = swap(take(pieces, other), "col")
    return states + side_by_side_members(kept, arrived, me)


def side_by_side_members(kept, arrived, me):
    first = jnp.where(me == 0, kept, arrived)
    second = jnp.where(me == 0, arrived, kept)
    return jnp.stack([first, second])


def solution(mesh):
    placed = (P("ens", None, ("row", "col")), P(("ens", "row"), "col"), P("ens", None))
    return jax.shard_map(
        advanced, mesh=mesh, in_specs=placed, out_specs=P("ens", None, ("row", "col")), check_vma=False
    )
```
